32 devices in a mesh: groups: 2 (over x), seq: 16 (over z, y, core).
Axes of the slice: x: 2, y: 2, z: 4, core: 2. Of those that a mesh axis runs over, the one named last changes fastest.
Arguments:
- queries: bfloat16 [4096, 1792], P(('groups', 'seq')), parts along dimension 0, may hold values from -100 to 100
- key_rows: bfloat16 [4096, 256], P(('groups', 'seq')), parts along dimension 0, may hold values from -100 to 100
- value_rows: bfloat16 [4096, 256], P(('groups', 'seq')), parts along dimension 0, may hold values from -6 to 6
- span_order: int32 [64], P('groups'), parts along dimension 0, may hold values from 0 to 31, each once
- kept_blocks: int32 [4, 1], P('groups'), parts along dimension 0, may hold values from 0 to 3, as said below
Outputs:
- attended: bfloat16 [4096, 1792], P(('groups', 'seq')), parts along dimension 0
- kept_cache: bfloat16 [1024, 512], P(('groups', 'seq')), parts along dimension 0
The draws below stay inside these ranges and needn't reach their ends.
There are 2 independent parts, one for each index of `groups`. The reference program is written for one: setup_inputs(seed, part) draws one part's arguments, and reference() takes and returns one part's arrays. A program takes and returns all parts, laid end to end along the dimension named above; each array names one. Nothing has to cross between parts.
Inputs may be any that keep to these rules, and one draw needn't show every extreme that they name: `kept_blocks`: each row lists 1 different blocks.
All inputs are finite; a program needn't handle non-finite values.
Results may differ from the reference program's by a relative error of at most 0.0055.
Values may be sent and summed in bfloat16 or wider, within the bound.
A program may use at most 64 MiB of HBM per device.

```python
import math
import jax
import jax.numpy as jnp
from jax import lax

HEAD_DIM = 128
Q_HEADS = 14
KV_HEADS = 2
GROUP = 7
TOK_DEV = 128
TOKENS = 2048
SPANS = 32
BLOCK = 512
NBLOCKS = 4
KEEP = 1
CACHE_ROWS = 512


def joint_draw(key):
    key_query = jax.random.fold_in(key, 101)
    key_keys = jax.random.fold_in(key, 102)
    query_part = jnp.clip(jax.random.normal(key_query, (TOKENS, KV_HEADS, GROUP, HEAD_DIM)), -6.0, 6.0)
    key_part = jnp.clip(jax.random.normal(key_keys, (TOKENS, KV_HEADS, HEAD_DIM)), -6.0, 6.0)
    return (query_part.reshape(TOKENS, Q_HEADS * HEAD_DIM), key_part.reshape(TOKENS, KV_HEADS * HEAD_DIM))


def draw_queries(key, part):
    query_part, key_part = joint_draw(key)
    return query_part.astype(jnp.bfloat16)


def draw_key_rows(key, part):
    query_part, key_part = joint_draw(key)
    return key_part.astype(jnp.bfloat16)


def draw_kept_blocks(key, part):
    shuffled = jax.random.permutation(jax.random.fold_in(key, 300), NBLOCKS).astype(jnp.int32)
    picks = (jnp.arange(KV_HEADS, dtype=jnp.int32)[:, None] * KEEP + jnp.arange(KEEP, dtype=jnp.int32)[None, :]) % NBLOCKS
    return shuffled[picks].astype(jnp.int32)


def block_scale(key, dims, cuts, smallest, top_value):
    factor_of, own = 1.0, jax.random.fold_in(key, 6)
    for position, parts in cuts:
        draws = jnp.exp(jax.random.uniform(jax.random.fold_in(own, position), (parts,), jnp.float32, smallest / len(cuts), top_value / len(cuts)))
        factor_of = factor_of * jnp.repeat(draws, dims[position] // parts).reshape([-1 if axis == position else 1 for axis in range(len(dims))])
    return factor_of


def bell_draw(own_key, extent, width, reach, split=(), kind=jnp.bfloat16):
    entries = width * jax.random.normal(own_key, extent, jnp.float32)
    if split:
        entries = entries * block_scale(own_key, extent, split, -0.22, 0.18)
    return jnp.clip(entries, -reach, reach).astype(kind)


def setup_inputs(seed: int = 0, part: int = 0) -> dict:
    splits = jax.random.split(jax.random.key(seed), 6)
    part_keys = jax.random.split(jax.random.fold_in(splits[5], part), 6)
    return {
        "queries": draw_queries(jax.random.fold_in(jax.random.fold_in(splits[5], part), 71), part),
        "key_rows": draw_key_rows(jax.random.fold_in(jax.random.fold_in(splits[5], part), 71), part),
        "value_rows": bell_draw(part_keys[2], (TOKENS, KV_HEADS * HEAD_DIM), 1.0, 6.0, ((0, 16),)),
        "span_order": jax.random.permutation(part_keys[3], SPANS).astype(jnp.int32),
        "kept_blocks": draw_kept_blocks(jax.random.fold_in(jax.random.fold_in(splits[5], part), 71), part),
    }


def token_positions(span_order, span_len):
    within = jnp.arange(span_len, dtype=jnp.int32)
    return (span_order.astype(jnp.int32)[:, None] * span_len + within[None, :]).reshape(-1).astype(jnp.int32)

def cache_sources(kept_blocks, row_ids):
    block_ids = row_ids // BLOCK
    match = jnp.arange(kept_blocks.shape[1], dtype=jnp.int32)[None, None, :] == block_ids[None, :, None]
    chosen = lax.optimization_barrier(jnp.sum(jnp.where(match, kept_blocks.astype(jnp.int32)[:, None, :], 0), axis=-1))
    return (chosen * BLOCK + row_ids[None, :] % BLOCK).astype(jnp.int32)

def reference(queries, key_rows, value_rows, span_order, kept_blocks):
    positions = token_positions(span_order, TOK_DEV // 2)
    scale = 1.0 / math.sqrt(HEAD_DIM)
    query_heads = queries.reshape(TOKENS, KV_HEADS, GROUP, HEAD_DIM)
    key_heads = key_rows.reshape(TOKENS, KV_HEADS, HEAD_DIM)
    value_heads = value_rows.reshape(TOKENS, KV_HEADS, HEAD_DIM)
    query_block = math.gcd(TOKENS, 512)
    query_blocks = TOKENS // query_block

    def one_block(index):
        index = index.astype(jnp.int32)
        head_index = (index // query_blocks).astype(jnp.int32)
        row_start = (index % query_blocks * query_block).astype(jnp.int32)
        zero_index = jnp.zeros((), jnp.int32)
        block_queries = lax.dynamic_slice(query_heads, (row_start, head_index, zero_index, zero_index), (query_block, 1, GROUP, HEAD_DIM))[:, 0]
        head_keys = lax.dynamic_index_in_dim(key_heads, head_index, 1, keepdims=False)
        head_values = lax.dynamic_index_in_dim(value_heads, head_index, 1, keepdims=False)
        block_pos = lax.dynamic_slice_in_dim(positions, row_start, query_block)
        scores = jnp.einsum('qgd,kd->gqk', block_queries.astype(jnp.float32), head_keys.astype(jnp.float32)) * scale
        visible = positions[None, None, :] <= block_pos[None, :, None]
        scores = jnp.where(visible, scores, -1e+30)
        row_max = lax.optimization_barrier(jnp.max(scores, axis=-1))
        weights = jnp.where(visible, jnp.exp(scores - row_max[..., None]), 0.0)
        totals = lax.optimization_barrier(jnp.sum(weights, axis=-1))
        rounded = weights.astype(jnp.bfloat16)
        mixed = jnp.einsum('gqk,kd->gqd', rounded.astype(jnp.float32), head_values.astype(jnp.float32)) / totals[..., None]
        return jnp.transpose(mixed, (1, 0, 2)).astype(jnp.bfloat16)
    results = lax.map(one_block, jnp.arange(KV_HEADS * query_blocks, dtype=jnp.int32))
    attended = results.reshape(KV_HEADS, query_blocks, query_block, GROUP, HEAD_DIM)
    attended = jnp.transpose(attended, (1, 2, 0, 3, 4)).reshape(TOKENS, Q_HEADS * HEAD_DIM)
    natural = jnp.zeros((TOKENS, 2 * KV_HEADS * HEAD_DIM), jnp.bfloat16)
    natural = natural.at[positions].set(jnp.concatenate([key_rows, value_rows], axis=1))
    sources = cache_sources(kept_blocks, jnp.arange(CACHE_ROWS, dtype=jnp.int32))
    columns = []
    for part_index in range(2):
        for head_index in range(KV_HEADS):
            low_col = part_index * KV_HEADS * HEAD_DIM + head_index * HEAD_DIM
            columns.append(natural[sources[head_index], low_col:low_col + HEAD_DIM])
    kept_cache = jnp.concatenate(columns, axis=1)
    return (attended, kept_cache)
```

```python
import functools
import math

import jax
import jax.numpy as jnp
from jax import lax
from jax.experimental import pallas as pl
from jax.experimental.pallas import tpu as pltpu
from jax.sharding import PartitionSpec as P

HEAD_DIM = 128
BLOCK = 512


def token_positions(span_order, span_len):
    within = jnp.arange(span_len, dtype=jnp.int32)
    return (span_order[:, None] * span_len + within[None, :]).reshape(-1)


def cache_sources(kept_blocks, row_ids):
    block_ids = row_ids // BLOCK
    match = (
        jnp.arange(kept_blocks.shape[1], dtype=jnp.int32)[None, None, :] == block_ids[None, :, None]
    )
    chosen = jnp.sum(jnp.where(match, kept_blocks[:, None, :], 0), axis=-1)
    return chosen * BLOCK + row_ids[None, :] % BLOCK


def local_plain(queries, key_rows, value_rows, span_order, kept_blocks):
    seq_count = lax.axis_size("seq")
    my_index = lax.axis_index("seq")
    query_rows = queries.shape[0]
    kv_heads = key_rows.shape[1] // HEAD_DIM
    group_size = queries.shape[1] // key_rows.shape[1]
    scale = 1.0 / math.sqrt(HEAD_DIM)
    positions = token_positions(span_order, query_rows // 2)
    query_pos = lax.dynamic_slice_in_dim(positions, my_index * query_rows, query_rows)
    query_heads = queries.reshape(query_rows, kv_heads, group_size, HEAD_DIM)
    cache_local = kept_blocks.shape[1] * BLOCK // seq_count
    cache_src = cache_sources(
        kept_blocks, my_index * cache_local + jnp.arange(cache_local, dtype=jnp.int32)
    )

    def pick_rows(sources, key_part, value_part, part_pos):
        onehot = (sources[:, :, None] == part_pos[None, None, :]).astype(jnp.bfloat16)
        count = key_part.shape[0]
        out_rows = sources.shape[1]
        picked_keys = jnp.einsum(
            "hrk,khd->rhd",
            onehot,
            key_part.reshape(count, kv_heads, HEAD_DIM),
            preferred_element_type=jnp.float32,
        )
        picked_values = jnp.einsum(
            "hrk,khd->rhd",
            onehot,
            value_part.reshape(count, kv_heads, HEAD_DIM),
            preferred_element_type=jnp.float32,
        )
        return jnp.concatenate(
            [picked_keys.reshape(out_rows, -1), picked_values.reshape(out_rows, -1)], axis=1
        )

    def attend_block(state, block_keys, block_values, block_pos):
        running_max, totals, accum = (state[0], state[1], state[2])
        count = block_keys.shape[0]
        scores = (
            jnp.einsum(
                "qhgd,khd->hgqk",
                query_heads,
                block_keys.reshape(count, kv_heads, HEAD_DIM),
                preferred_element_type=jnp.float32,
            )
            * scale
        )
        visible = block_pos[None, None, None, :] <= query_pos[None, None, :, None]
        scores = jnp.where(visible, scores, -1e30)
        new_max = jnp.maximum(running_max, jnp.max(scores, axis=-1))
        weights = jnp.where(visible, jnp.exp(scores - new_max[..., None]), 0.0)
        factor = jnp.exp(running_max - new_max)
        totals = totals * factor + jnp.sum(weights, axis=-1)
        mixed = jnp.einsum(
            "hgqk,khd->hgqd",
            weights.astype(jnp.bfloat16),
            block_values.reshape(count, kv_heads, HEAD_DIM),
            preferred_element_type=jnp.float32,
        )
        accum = accum * factor[..., None] + mixed
        return (new_max, totals, accum)

    initial = (
        jnp.full((kv_heads, group_size, query_rows), -1e30, jnp.float32),
        jnp.zeros((kv_heads, group_size, query_rows), jnp.float32),
        jnp.zeros((kv_heads, group_size, query_rows, HEAD_DIM), jnp.float32),
    )
    initial = initial + (jnp.zeros((cache_local, 2 * kv_heads * HEAD_DIM), jnp.float32),)
    piece_keys = lax.all_gather(key_rows, "seq", axis=0, tiled=True)
    piece_values = lax.all_gather(value_rows, "seq", axis=0, tiled=True)
    count = piece_keys.shape[0]
    width = math.gcd(count, 512)

    def inner(step_index, inner_state):
        offset = (step_index * width).astype(jnp.int32)
        block_keys = lax.dynamic_slice_in_dim(piece_keys, offset, width, 0)
        block_values = lax.dynamic_slice_in_dim(piece_values, offset, width, 0)
        block_pos = lax.dynamic_slice_in_dim(positions, offset, width)
        updated = attend_block(inner_state, block_keys, block_values, block_pos)
        extra = (inner_state[3] + pick_rows(cache_src, block_keys, block_values, block_pos),)
        return updated + extra

    final = lax.fori_loop(0, count // width, inner, initial)
    attended = final[2] / final[1][..., None]
    attended = jnp.transpose(attended, (2, 0, 1, 3)).reshape(query_rows, -1).astype(jnp.bfloat16)
    kept_cache = final[3].astype(jnp.bfloat16)
    return (attended, kept_cache)

VMEM_BUDGET = 44 * 1024 * 1024
MASKED = -1e30


def ring_place(chip, chips):
    odd = chip % 2
    return (1 - odd) * (chip // 2) + odd * (chips - 1 - chip // 2)


def ring_chip(place, chips):
    back = place // (chips // 2)
    return (1 - back) * 2 * place + back * (2 * (chips - 1 - place) + 1)


def fused_kernel(
    chips,
    span_ref,
    kept_ref,
    q_ref,
    k_ref,
    v_ref,
    out_ref,
    cache_ref,
    k_all,
    v_all,
    scores,
    weights,
    row_max,
    send_sem,
    recv_sem,
):
    rows = k_ref.shape[0]
    span_len = rows // 2
    pair = 2 * rows
    kv_heads = k_ref.shape[1] // HEAD_DIM
    heads = q_ref.shape[1] // HEAD_DIM
    group = heads // kv_heads
    factor = math.log2(math.e) / math.sqrt(HEAD_DIM)

    me = lax.axis_index("seq")
    chip, core = me // 2, me % 2
    place = ring_place(chip, chips)
    partner = 2 * chip + 1 - core

    def chip_at(step):
        return ring_chip((place + step + 2 * chips) % chips, chips)

    right = 2 * chip_at(1) + core
    left = 2 * chip_at(-1) + core

    barrier = pltpu.get_barrier_semaphore()
    for other in (left, right, partner):
        pl.semaphore_signal(
            barrier, inc=1, device_id={"seq": other}, device_id_type=pl.DeviceIdType.MESH
        )
    pl.semaphore_wait(barrier, 3)

    long_way = chips // 2
    short_way = chips - 1 - long_way
    reach = {("k", 1): long_way, ("k", -1): short_way, ("v", 1): short_way, ("v", -1): long_way}
    own = {"k": k_ref, "v": v_ref}
    gathered = {"k": k_all, "v": v_all}
    counter = [0]

    def tile(kind, index):
        return gathered[kind].at[pl.ds(pl.multiple_of(index * rows, rows), rows), :]

    def message(kind, step, target):
        index = 2 * chip_at(step) + core
        slot = counter[0]
        counter[0] += 1
        return pltpu.make_async_remote_copy(
            src_ref=own[kind] if step == 0 else tile(kind, index),
            dst_ref=tile(kind, index),
            send_sem=send_sem.at[slot],
            recv_sem=recv_sem.at[slot],
            device_id={"seq": target},
            device_id_type=pl.DeviceIdType.MESH,
        )

    hops, crossings = {}, {}
    for kind in ("k", "v"):
        for way in (1, -1):
            for hop in range(1, reach[kind, way] + 1):
                hops[kind, way, hop] = message(kind, -way * (hop - 1), right if way == 1 else left)
        crossings[kind, 0] = message(kind, 0, partner)
        for way in (1, -1):
            for hop in range(1, reach[kind, way] + 1):
                crossings[kind, -way * hop] = message(kind, -way * hop, partner)

    for kind in ("k", "v"):
        hops[kind, 1, 1].start()
        hops[kind, -1, 1].start()
        crossings[kind, 0].start()

    def relay(kind, hop):
        for way in (1, -1):
            if hop <= reach[kind, way]:
                hops[kind, way, hop].wait_recv()
                if hop < reach[kind, way]:
                    hops[kind, way, hop + 1].start()
                crossings[kind, -way * hop].start()

    own_rows = pl.ds(pl.multiple_of(me * rows, rows), rows)
    k_all[own_rows, :] = k_ref[...]
    v_all[own_rows, :] = v_ref[...]

    row_ids = lax.broadcasted_iota(jnp.int32, (rows, pair), 0)
    key_ids = lax.broadcasted_iota(jnp.int32, (rows, pair), 1)
    query_pos = (
        jnp.where(row_ids < span_len, span_ref[2 * me], span_ref[2 * me + 1]) * span_len
        + row_ids % span_len
    )

    def score_chip(step):
        at = chip_at(step)
        s0, s1, s2, s3 = (span_ref[4 * at + i] for i in range(4))
        spans = jnp.where(
            key_ids < rows,
            jnp.where(key_ids < span_len, s0, s1),
            jnp.where(key_ids < rows + span_len, s2, s3),
        )
        key_pos = spans * span_len + key_ids % span_len
        bias = jnp.where(key_pos <= query_pos, 0.0, MASKED)
        key_rows = pl.ds(pl.multiple_of(at * pair, pair), pair)
        for h in range(kv_heads):
            keys = k_all[key_rows, h * HEAD_DIM : (h + 1) * HEAD_DIM]
            for g in range(group):
                j = h * group + g
                s = lax.dot_general(
                    q_ref[:, j * HEAD_DIM : (j + 1) * HEAD_DIM],
                    keys,
                    (((1,), (1,)), ((), ())),
                    preferred_element_type=jnp.float32,
                )
                s = s * factor + bias
                scores[j, :, key_rows] = s
                top = jnp.maximum(s[:, :rows], s[:, rows:])
                row_max[j] = top if step == 0 else jnp.maximum(row_max[j], top)

    crossings["k", 0].wait_recv()
    score_chip(0)
    for hop in range(1, long_way + 1):
        relay("k", hop)
        relay("v", hop)
        for way in (1, -1):
            if hop <= reach["k", way]:
                crossings["k", -way * hop].wait_recv()
                score_chip(-way * hop)

    for j in range(heads):
        top = jnp.max(row_max[j], axis=1, keepdims=True)
        weights[j] = jnp.exp2(scores[j] - top).astype(jnp.bfloat16)

    for step in range(-(chips - 1), chips):
        if ("v", step) in crossings:
            crossings["v", step].wait_recv()

    cache_rows = cache_ref.shape[0]
    first = me * cache_rows
    within = pl.multiple_of(first % span_len, cache_rows)
    for h in range(kv_heads):
        span = kept_ref[h, first // BLOCK] * (BLOCK // span_len) + first % BLOCK // span_len
        columns = slice(h * HEAD_DIM, (h + 1) * HEAD_DIM)
        later = slice((kv_heads + h) * HEAD_DIM, (kv_heads + h + 1) * HEAD_DIM)
        picked_keys = jnp.zeros((cache_rows, HEAD_DIM), jnp.float32)
        picked_values = jnp.zeros((cache_rows, HEAD_DIM), jnp.float32)
        for s in range(span_ref.shape[0]):
            chosen = jnp.where(span_ref[s] == span, 1.0, 0.0)
            source = pl.ds(s * span_len + within, cache_rows)
            picked_keys += k_all[source, columns].astype(jnp.float32) * chosen
            picked_values += v_all[source, columns].astype(jnp.float32) * chosen
        cache_ref[:, columns] = picked_keys.astype(cache_ref.dtype)
        cache_ref[:, later] = picked_values.astype(cache_ref.dtype)

    ones = jnp.ones((v_all.shape[0], HEAD_DIM), jnp.bfloat16)
    for h in range(kv_heads):
        values = jnp.concatenate([v_all[:, h * HEAD_DIM : (h + 1) * HEAD_DIM], ones], axis=1)
        for g in range(group):
            j = h * group + g
            mixed = jnp.dot(weights[j], values, preferred_element_type=jnp.float32)
            out_ref[:, j * HEAD_DIM : (j + 1) * HEAD_DIM] = (
                mixed[:, :HEAD_DIM] / mixed[:, HEAD_DIM:]
            ).astype(out_ref.dtype)

    for copy in (*hops.values(), *crossings.values()):
        copy.wait_send()


def local(queries, key_rows, value_rows, span_order, kept_blocks):
    seq_count = lax.axis_size("seq")
    rows = key_rows.shape[0]
    heads = queries.shape[1] // HEAD_DIM
    tokens = rows * seq_count
    cache_local = kept_blocks.shape[1] * BLOCK // seq_count
    span_len = rows // 2
    fits = heads * rows * tokens * 6 + 4 * tokens * key_rows.shape[1] <= VMEM_BUDGET
    if not fits or seq_count < 8 or span_len % cache_local or cache_local % 16:
        return local_plain(queries, key_rows, value_rows, span_order, kept_blocks)
    chips = seq_count // 2
    messages = 2 * (2 * chips - 1)
    vmem = pl.BlockSpec(memory_space=pltpu.VMEM)
    smem = pl.BlockSpec(memory_space=pltpu.SMEM)
    return pl.pallas_call(
        functools.partial(fused_kernel, chips),
        out_shape=(
            jax.ShapeDtypeStruct(queries.shape, jnp.bfloat16),
            jax.ShapeDtypeStruct((cache_local, 2 * key_rows.shape[1]), jnp.bfloat16),
        ),
        in_specs=[smem, smem, vmem, vmem, vmem],
        out_specs=(vmem, vmem),
        scratch_shapes=[
            pltpu.VMEM((tokens, key_rows.shape[1]), jnp.bfloat16),
            pltpu.VMEM((tokens, key_rows.shape[1]), jnp.bfloat16),
            pltpu.VMEM((heads, rows, tokens), jnp.float32),
            pltpu.VMEM((heads, rows, tokens), jnp.bfloat16),
            pltpu.VMEM((heads, rows, HEAD_DIM), jnp.float32),
            pltpu.SemaphoreType.DMA((messages,)),
            pltpu.SemaphoreType.DMA((messages,)),
        ],
        compiler_params=pltpu.CompilerParams(
            collective_id=0, has_side_effects=True, vmem_limit_bytes=60 * 1024 * 1024
        ),
    )(span_order, kept_blocks, queries, key_rows, value_rows)


def solution(mesh):
    placed = (
        P(("groups", "seq"), None),
        P(("groups", "seq"), None),
        P(("groups", "seq"), None),
        P("groups"),
        P("groups", None),
    )
    return jax.shard_map(
        local,
        mesh=mesh,
        in_specs=placed,
        out_specs=(P(("groups", "seq"), None), P(("groups", "seq"), None)),
        check_vma=False,
    )
```
